32 devices in a mesh: shard: 8 (over z, y), tp: 4 (over x, core).
Axes of the slice: x: 2, y: 2, z: 4, core: 2. Of those that a mesh axis runs over, the one named last changes fastest.
Arguments:
- train_query: bfloat16 [8192, 8192], P('shard', 'tp'), may hold values from -0.0625 to 0.0625
- low_query: bfloat16 [8192, 16], P('shard'), may hold values from -0.0625 to 0.0625
- high_query: bfloat16 [16, 8192], P(None, 'tp'), may hold values from -1.5 to 1.5
- train_key: bfloat16 [8192, 1024], P('shard', 'tp'), may hold values from -0.0625 to 0.0625
- low_key: bfloat16 [8192, 16], P('shard'), may hold values from -0.0625 to 0.0625
- high_key: bfloat16 [16, 1024], P(None, 'tp'), may hold values from -1.5 to 1.5
- train_value: bfloat16 [8192, 1024], P('shard', 'tp'), may hold values from -0.0625 to 0.0625
- low_value: bfloat16 [8192, 16], P('shard'), may hold values from -0.0625 to 0.0625
- high_value: bfloat16 [16, 1024], P(None, 'tp'), may hold values from -1.5 to 1.5
- norm_train: float32 [8192], P(('shard', 'tp')), may hold values from 0.25 to 1.75
- norm_step: float32 [8192], P(('shard', 'tp')), may hold values from -0.3 to 0.3
Outputs:
- serving_query: bfloat16 [8192, 8192], P('tp')
- serving_key: bfloat16 [1024, 8192], P('tp')
- serving_value: bfloat16 [1024, 8192], P('tp')
- serve_norm: bfloat16 [8192], replicated
The draws below stay inside these ranges and needn't reach their ends.
All inputs are finite; a program needn't handle non-finite values.
Results may differ from the reference program's by a relative error of at most 0.001.
Values may be sent and summed in bfloat16 or wider, within the bound.
A program may use at most 128 MiB of HBM per device.

```python
import jax
import jax.numpy as jnp

D_MODEL = 8192
Q_DIM = 8192
KV_DIM = 1024
RANK = 16


def shard_levels(key, extent, pieces, smallest, top_value):
    factor_of, own = 1.0, jax.random.fold_in(key, 6)
    for position, blocks in pieces:
        heights = jnp.exp(jax.random.uniform(jax.random.fold_in(own, position), (blocks,), jnp.float32, smallest / len(pieces), top_value / len(pieces)))
        factor_of = factor_of * jnp.repeat(heights, extent[position] // blocks).reshape([-1 if axis == position else 1 for axis in range(len(extent))])
    return factor_of


def normal_values(key, extent, deviation, bound, cuts=(), dtype=jnp.bfloat16):
    loudness = shard_levels(key, extent, cuts, -0.22, 0.18) if cuts else 1.0
    entries = jax.random.normal(key, extent, jnp.float32) * deviation * loudness
    return jnp.minimum(jnp.maximum(entries, -bound), bound).astype(dtype)


def setup_inputs(seed: int = 0) -> dict:
    streams_of = jax.random.split(jax.random.key(seed), 12)
    train_query = normal_values(streams_of[0], (D_MODEL, Q_DIM), D_MODEL ** -0.5, 0.0625, ((0, 8), (1, 4)))
    low_query = normal_values(streams_of[1], (D_MODEL, RANK), D_MODEL ** -0.5, 0.0625, ((0, 8),))
    high_query = normal_values(streams_of[2], (RANK, Q_DIM), RANK ** -0.5, 1.5, ((1, 4),))
    train_key = normal_values(streams_of[3], (D_MODEL, KV_DIM), D_MODEL ** -0.5, 0.0625, ((0, 8), (1, 4)))
    low_key = normal_values(streams_of[4], (D_MODEL, RANK), D_MODEL ** -0.5, 0.0625, ((0, 8),))
    high_key = normal_values(streams_of[5], (RANK, KV_DIM), RANK ** -0.5, 1.5, ((1, 4),))
    train_value = normal_values(streams_of[6], (D_MODEL, KV_DIM), D_MODEL ** -0.5, 0.0625, ((0, 8), (1, 4)))
    low_value = normal_values(streams_of[7], (D_MODEL, RANK), D_MODEL ** -0.5, 0.0625, ((0, 8),))
    high_value = normal_values(streams_of[8], (RANK, KV_DIM), RANK ** -0.5, 1.5, ((1, 4),))
    norm_train = jnp.clip(1.0 + 0.15 * jax.random.normal(streams_of[9], (D_MODEL,), jnp.float32), 0.25, 1.75)
    norm_step = jnp.clip(jax.random.uniform(streams_of[10], (D_MODEL,), jnp.float32, -0.3, 0.3) * shard_levels(streams_of[10], (D_MODEL,), ((0, 32),), -0.4, 0.0), -0.3, 0.3)
    return {"train_query": train_query, "low_query": low_query, "high_query": high_query, "train_key": train_key, "low_key": low_key, "high_key": high_key, "train_value": train_value, "low_value": low_value, "high_value": high_value, "norm_train": norm_train, "norm_step": norm_step}


mix_rate = 0.5


def reference(train_query, low_query, high_query, train_key, low_key, high_key, train_value, low_value, high_value, norm_train, norm_step):
    whole_query = train_query.astype(jnp.float32) + mix_rate * jnp.dot(low_query, high_query, preferred_element_type=jnp.float32)
    whole_key = train_key.astype(jnp.float32) + mix_rate * jnp.dot(low_key, high_key, preferred_element_type=jnp.float32)
    whole_value = train_value.astype(jnp.float32) + mix_rate * jnp.dot(low_value, high_value, preferred_element_type=jnp.float32)
    serving_query = whole_query.T.astype(jnp.bfloat16)
    serving_key = whole_key.T.astype(jnp.bfloat16)
    serving_value = whole_value.T.astype(jnp.bfloat16)
    serve_norm = (norm_train + norm_step).astype(jnp.bfloat16)
    return serving_query, serving_key, serving_value, serve_norm
```

```python
import functools

import jax
import jax.numpy as jnp
from jax import lax
from jax.experimental import pallas as pl
from jax.experimental.pallas import tpu as pltpu
from jax.sharding import PartitionSpec as P

mix_rate = 0.5


def merge(train, low, high):
    whole = train.astype(jnp.float32) + mix_rate * jnp.dot(
        low, high, preferred_element_type=jnp.float32
    )
    return whole.astype(jnp.bfloat16)


def place_kernel(where_ref, block_ref, *refs):
    refs[-1][...] = block_ref[...].T


def place(block, out, where, total):
    rows, columns = block.shape
    tile = min(columns, 512)
    fixed = [] if out is None else [out]
    return pl.pallas_call(
        place_kernel,
        out_shape=jax.ShapeDtypeStruct((columns, total), block.dtype),
        grid_spec=pltpu.PrefetchScalarGridSpec(
            num_scalar_prefetch=1,
            grid=(columns // tile,),
            in_specs=[pl.BlockSpec((rows, tile), lambda i, where_ref: (0, i))]
            + [pl.BlockSpec(memory_space=pl.ANY)] * len(fixed),
            out_specs=pl.BlockSpec((tile, rows), lambda i, where_ref: (i, where_ref[0])),
        ),
        input_output_aliases={2: 0} if fixed else {},
        cost_estimate=pl.CostEstimate(
            flops=0, bytes_accessed=4 * rows * columns, transcendentals=0
        ),
    )(where.reshape(1), block, *fixed)


def per_device(
    count,
    train_query,
    low_query,
    high_query,
    train_key,
    low_key,
    high_key,
    train_value,
    low_value,
    high_value,
    norm_train,
    norm_step,
):
    cycle = list(range(0, count, 2)) + list(range(1, count, 2))[::-1]
    ahead = [(cycle[i], cycle[(i + 1) % count]) for i in range(count)]
    behind = [(to, start) for start, to in ahead]
    me = lax.axis_index("shard")
    spot_of = [cycle.index(i) for i in range(count)]
    spot = jnp.asarray(spot_of, jnp.int32)[me]
    at_spot = jnp.asarray(cycle, jnp.int32)

    rows = train_query.shape[0]
    half = rows // 2
    own = {
        "qa": merge(train_query[:half], low_query[:half], high_query),
        "qb": merge(train_query[half:], low_query[half:], high_query),
        "k": merge(train_key, low_key, high_key),
        "v": merge(train_value, low_value, high_value),
    }
    outs = {"q": None, "k": None, "v": None}
    total = rows * count

    def settle(name, block, owner):
        if name == "qa" or name == "qb":
            where = owner * 2 + (1 if name == "qb" else 0)
        else:
            where = owner
        outs[name[0]] = place(block, outs[name[0]], where, total)

    right, left = dict(own), dict(own)
    middle = count // 2
    arrivals = []
    for step in range(1, middle + 1):
        last = step == middle and count % 2 == 0
        right_names = ("k", "qa") if last else ("qa", "qb", "k", "v")
        left_names = ("v", "qb") if last else ("qb", "qa", "v", "k")
        right = {name: lax.ppermute(right[name], "shard", ahead) for name in right_names}
        left = {name: lax.ppermute(left[name], "shard", behind) for name in left_names}
        arrivals.append((step, right, left))

    for name, block in own.items():
        settle(name, block, me)
    for step, right, left in arrivals:
        from_right = at_spot[(spot - step + count) % count]
        from_left = at_spot[(spot + step) % count]
        for name_right, name_left in zip(right, left):
            settle(name_right, right[name_right], from_right)
            settle(name_left, left[name_left], from_left)

    serve_norm = lax.all_gather(
        (norm_train + norm_step).astype(jnp.bfloat16), ("shard", "tp"), axis=0, tiled=True
    )
    return (outs["q"], outs["k"], outs["v"], serve_norm)


def solution(mesh):
    in_specs = (
        P("shard", "tp"),
        P("shard", None),
        P(None, "tp"),
        P("shard", "tp"),
        P("shard", None),
        P(None, "tp"),
        P("shard", "tp"),
        P("shard", None),
        P(None, "tp"),
        P(("shard", "tp")),
        P(("shard", "tp")),
    )
    out_specs = (P("tp", None), P("tp", None), P("tp", None), P())
    return jax.shard_map(
        functools.partial(per_device, mesh.shape["shard"]),
        mesh=mesh,
        in_specs=in_specs,
        out_specs=out_specs,
        check_vma=False,
    )
```

```python
import functools

import jax
import jax.numpy as jnp
from jax import lax
from jax.experimental import pallas as pl
from jax.experimental.pallas import tpu as pltpu
from jax.sharding import PartitionSpec as P

mix_rate = 0.5


def merge(train, low, high):
    whole = train.astype(jnp.float32) + mix_rate * jnp.dot(
        low, high, preferred_element_type=jnp.float32
    )
    return whole.astype(jnp.bfloat16)


def place(block, out, where, total, riders):
    rows, columns = block.shape
    tile = min(columns, 512)
    fixed = [] if out is None else [out]
    first = len(fixed)
    aliases = {2: 0} if fixed else {}
    aliases.update({2 + first + i: 1 + i for i in range(len(riders))})
    spot = first + len(riders)

    def kernel(where_ref, block_ref, *refs):
        refs[spot][...] = block_ref[...].T

    placed = pl.pallas_call(
        kernel,
        out_shape=[jax.ShapeDtypeStruct((columns, total), block.dtype)]
        + [jax.ShapeDtypeStruct(rider.shape, rider.dtype) for rider in riders],
        grid_spec=pltpu.PrefetchScalarGridSpec(
            num_scalar_prefetch=1,
            grid=(columns // tile,),
            in_specs=[pl.BlockSpec((rows, tile), lambda i, where_ref: (0, i))]
            + [pl.BlockSpec(memory_space=pl.ANY)] * spot,
            out_specs=[pl.BlockSpec((tile, rows), lambda i, where_ref: (i, where_ref[0]))]
            + [pl.BlockSpec(memory_space=pl.ANY)] * len(riders),
        ),
        input_output_aliases=aliases,
        cost_estimate=pl.CostEstimate(
            flops=0, bytes_accessed=4 * rows * columns, transcendentals=0
        ),
    )(where.reshape(1), block, *fixed, *riders)
    return placed[0], placed[1:]


def per_device(
    count,
    train_query,
    low_query,
    high_query,
    train_key,
    low_key,
    high_key,
    train_value,
    low_value,
    high_value,
    norm_train,
    norm_step,
):
    cycle = list(range(0, count, 2)) + list(range(1, count, 2))[::-1]
    ahead = [(cycle[i], cycle[(i + 1) % count]) for i in range(count)]
    behind = [(to, start) for start, to in ahead]
    me = lax.axis_index("shard")
    spot_of = [cycle.index(i) for i in range(count)]
    spot = jnp.asarray(spot_of, jnp.int32)[me]
    at_spot = jnp.asarray(cycle, jnp.int32)

    rows = train_query.shape[0]
    half = rows // 2
    own = {
        "qa": merge(train_query[:half], low_query[:half], high_query),
        "qb": merge(train_query[half:], low_query[half:], high_query),
        "k": merge(train_key, low_key, high_key),
        "v": merge(train_value, low_value, high_value),
    }
    outs = {"q": None, "k": None, "v": None}
    total = rows * count

    def settle(name, block, owner, riders=()):
        where = owner * 2 + (name == "qb") if name in ("qa", "qb") else owner
        outs[name[0]], passed = place(block, outs[name[0]], where, total, list(riders))
        return passed

    middle = count // 2
    units = []
    for step in range(1, middle + 1):
        if step == middle and count % 2 == 0:
            pairs = (("qa", "qb"), ("k", "v"))
        else:
            pairs = (("qa", "qb"), ("qb", "qa"), ("k", "v"), ("v", "k"))
        units += [(step, *pair) for pair in pairs]

    def send(unit, right, left):
        arrived[unit] = (lax.ppermute(right, "shard", ahead), lax.ppermute(left, "shard", behind))

    arrived = {}
    for unit in units:
        if unit[0] == 1:
            send(unit, own[unit[1]], own[unit[2]])

    def settle_both(names, blocks, owners, following, extra=()):
        onward = following and (following[0] + 1, *following[1:])
        riders = arrived[following] if onward in units else None
        passed = settle(names[0], blocks[0], owners[0], [*(riders or ())[:1], *extra])
        passed_left = settle(names[1], blocks[1], owners[1], (riders or ())[1:])
        if riders:
            arrived[following] = (passed[0], passed_left[0])
            send(onward, *arrived[following])
        return passed

    norm = (norm_train + norm_step).reshape(1, -1)
    settle("qa", own["qa"], me)
    (norm,) = settle("qb", own["qb"], me, [norm])
    serve_norm = lax.all_gather(
        norm.reshape(-1).astype(jnp.bfloat16), ("shard", "tp"), axis=0, tiled=True
    )
    passed = settle_both(
        ("k", "v"), (own["k"], own["v"]), (me, me), units[0], [serve_norm.reshape(1, -1)]
    )
    serve_norm = passed[-1].reshape(-1)
    for position, unit in enumerate(units):
        step = unit[0]
        owners = (at_spot[(spot - step + count) % count], at_spot[(spot + step) % count])
        following = units[position + 1] if position + 1 < len(units) else None
        settle_both(unit[1:], arrived[unit], owners, following)
    return (outs["q"], outs["k"], outs["v"], serve_norm)


def solution(mesh):
    in_specs = (
        P("shard", "tp"),
        P("shard", None),
        P(None, "tp"),
        P("shard", "tp"),
        P("shard", None),
        P(None, "tp"),
        P("shard", "tp"),
        P("shard", None),
        P(None, "tp"),
        P(("shard", "tp")),
        P(("shard", "tp")),
    )
    out_specs = (P("tp", None), P("tp", None), P("tp", None), P())
    return jax.shard_map(
        functools.partial(per_device, mesh.shape["shard"]),
        mesh=mesh,
        in_specs=in_specs,
        out_specs=out_specs,
        check_vma=False,
    )
```

```python
import functools

import jax
import jax.numpy as jnp
from jax import lax
from jax.experimental import pallas as pl
from jax.experimental.pallas import tpu as pltpu
from jax.sharding import PartitionSpec as P

mix_rate = 0.5


def merge(train, low, high):
    whole = train.astype(jnp.float32) + mix_rate * jnp.dot(
        low, high, preferred_element_type=jnp.float32
    )
    return whole.astype(jnp.bfloat16)


def place(block, out, where, total, riders):
    rows, columns = block.shape
    tile = min(columns, 512)
    fixed = [] if out is None else [out]
    first = len(fixed)
    aliases = {2: 0} if fixed else {}
    aliases.update({2 + first + i: 1 + i for i in range(len(riders))})
    spot = first + len(riders)

    def kernel(where_ref, block_ref, *refs):
        refs[spot][...] = block_ref[...].T

    placed = pl.pallas_call(
        kernel,
        out_shape=[jax.ShapeDtypeStruct((columns, total), block.dtype)]
        + [jax.ShapeDtypeStruct(rider.shape, rider.dtype) for rider in riders],
        grid_spec=pltpu.PrefetchScalarGridSpec(
            num_scalar_prefetch=1,
            grid=(columns // tile,),
            in_specs=[pl.BlockSpec((rows, tile), lambda i, where_ref: (0, i))]
            + [pl.BlockSpec(memory_space=pl.ANY)] * spot,
            out_specs=[pl.BlockSpec((tile, rows), lambda i, where_ref: (i, where_ref[0]))]
            + [pl.BlockSpec(memory_space=pl.ANY)] * len(riders),
        ),
        input_output_aliases=aliases,
        cost_estimate=pl.CostEstimate(
            flops=0, bytes_accessed=4 * rows * columns, transcendentals=0
        ),
    )(where.reshape(1), block, *fixed, *riders)
    return placed[0], placed[1:]


def per_device(
    count,
    train_query,
    low_query,
    high_query,
    train_key,
    low_key,
    high_key,
    train_value,
    low_value,
    high_value,
    norm_train,
    norm_step,
):
    cycle = list(range(0, count, 2)) + list(range(1, count, 2))[::-1]
    ahead = [(cycle[i], cycle[(i + 1) % count]) for i in range(count)]
    behind = [(to, start) for start, to in ahead]
    me = lax.axis_index("shard")
    spot_of = [cycle.index(i) for i in range(count)]
    spot = jnp.asarray(spot_of, jnp.int32)[me]
    at_spot = jnp.asarray(cycle, jnp.int32)

    rows = train_query.shape[0]
    half = rows // 2
    own = {
        "qa": merge(train_query[:half], low_query[:half], high_query),
        "qb": merge(train_query[half:], low_query[half:], high_query),
        "k": merge(train_key, low_key, high_key),
        "v": merge(train_value, low_value, high_value),
    }
    outs = {"q": None, "k": None, "v": None}
    total = rows * count

    def settle(name, block, owner, riders=()):
        where = owner * 2 + (name == "qb") if name in ("qa", "qb") else owner
        outs[name[0]], passed = place(block, outs[name[0]], where, total, list(riders))
        return passed

    middle = count // 2
    units = []
    for step in range(1, middle + 1):
        if step == middle and count % 2 == 0:
            pairs = (("qa", "qb"), ("k", "v"))
        else:
            pairs = (("qa", "qb"), ("qb", "qa"), ("k", "v"), ("v", "k"))
        units += [(step, *pair) for pair in pairs]

    def send(unit, right, left):
        arrived[unit] = (lax.ppermute(right, "shard", ahead), lax.ppermute(left, "shard", behind))

    arrived = {}
    for unit in units:
        if unit[0] == 1:
            send(unit, own[unit[1]], own[unit[2]])

    def settle_both(names, blocks, owners, following, extra=()):
        onward = following and (following[0] + 1, *following[1:])
        riders = arrived[following] if onward in units else None
        passed = settle(names[0], blocks[0], owners[0], [*(riders or ())[:1], *extra])
        passed_left = settle(names[1], blocks[1], owners[1], (riders or ())[1:])
        if riders:
            arrived[following] = (passed[0], passed_left[0])
            send(onward, *arrived[following])
        return passed

    norm = (norm_train + norm_step).reshape(1, -1)
    settle("qa", own["qa"], me)
    (norm,) = settle("qb", own["qb"], me, [norm])
    row = lax.all_gather(norm.reshape(-1).astype(jnp.bfloat16), "tp", axis=0, tiled=True)
    passed = settle_both(
        ("k", "v"), (own["k"], own["v"]), (me, me), units[0], [row.reshape(1, -1)]
    )
    row = passed[-1]

    def place_row(block, owner):
        return lax.dynamic_update_slice(serve_norm, block, (owner, 0))

    serve_norm = jnp.zeros((count, row.shape[1]), row.dtype)
    serve_norm = place_row(row, me)
    tiny, seen = (row, row), 0
    for position, unit in enumerate(units):
        step = unit[0]
        owners = (at_spot[(spot - step + count) % count], at_spot[(spot + step) % count])
        following = units[position + 1] if position + 1 < len(units) else None
        extra = ()
        if step != seen:
            extra = [
                lax.ppermute(tiny[0], "shard", ahead),
                lax.ppermute(tiny[1], "shard", behind),
            ]
        passed = settle_both(unit[1:], arrived[unit], owners, following, extra)
        if step != seen:
            tiny, seen = passed[-2:], step
            serve_norm = place_row(tiny[0], owners[0])
            serve_norm = place_row(tiny[1], owners[1])
    serve_norm = serve_norm.reshape(-1)
    return (outs["q"], outs["k"], outs["v"], serve_norm)


def solution(mesh):
    in_specs = (
        P("shard", "tp"),
        P("shard", None),
        P(None, "tp"),
        P("shard", "tp"),
        P("shard", None),
        P(None, "tp"),
        P("shard", "tp"),
        P("shard", None),
        P(None, "tp"),
        P(("shard", "tp")),
        P(("shard", "tp")),
    )
    out_specs = (P("tp", None), P("tp", None), P("tp", None), P())
    return jax.shard_map(
        functools.partial(per_device, mesh.shape["shard"]),
        mesh=mesh,
        in_specs=in_specs,
        out_specs=out_specs,
        check_vma=False,
    )
```
